32 devices in a mesh: groups: 2 (over y), expert: 4 (over x, core), cuts: 4 (over z).
Axes of the slice: x: 2, y: 2, z: 4, core: 2. Of those that a mesh axis runs over, the one named last changes fastest.
Arguments:
- tokens: bfloat16 [4096, 2048], P(('groups', 'expert')), parts along dimension 0, may hold values from -6 to 6
- route: int32 [4096, 1], P(('groups', 'expert')), parts along dimension 0, may hold values from 0 to 3; in each aligned block of 512 rows (0 to 511, 512 to 1023, ...) at most 192 rows name the same one
- gate_prob: float32 [4096], P(('groups', 'expert')), parts along dimension 0, may hold values from 0.2 to 1
- norm_gain: float32 [2048], replicated, may hold values from 0.5 to 1.5
- dense_in: bfloat16 [2048, 8192], P('expert', 'cuts'), may hold values from -0.125 to 0.125
- dense_out: bfloat16 [8192, 2048], P('cuts', 'expert'), may hold values from -0.0625 to 0.0625
- expert_in: bfloat16 [4, 2048, 8192], P('expert', None, 'cuts'), may hold values from -0.125 to 0.125
- expert_out: bfloat16 [4, 8192, 2048], P('expert', 'cuts'), may hold values from -0.0625 to 0.0625
Outputs:
- layer_out: bfloat16 [4096, 2048], P(('groups', 'expert'), 'cuts'), parts along dimension 0
The draws below stay inside these ranges and needn't reach their ends.
There are 2 independent parts, one for each index of `groups`. The reference program is written for one: setup_inputs(seed, part) draws one part's arguments, and reference() takes and returns one part's arrays. A program takes and returns all parts, laid end to end along the dimension named above; an argument that names none is the same for every part. Nothing has to cross between parts.
Inputs may be any that keep to these rules, and one draw needn't show every extreme that they name: `route`: within the rows of one device (aligned blocks of 512 rows) no expert is named by more than 192 rows; in some blocks one expert is named by exactly 192 rows.
All inputs are finite; a program needn't handle non-finite values.
Results may differ from the reference program's by a relative error of at most 0.0095.
Values may be sent and summed in bfloat16 or wider, within the bound.
A program may use at most 128 MiB of HBM per device.

```python
import math
import jax
import jax.numpy as jnp
import numpy as np
from jax import lax

D = 2048
FF = 8192
TOK_E = 512
EXPERTS = 4
CAP = 192
TOKENS = 2048
N_EXPERT = 4
N_CUTS = 4


def levels(stream_key, dims, shards, least, top_value):
    def one(dim, shards_of):
        draws = jax.random.uniform(jax.random.fold_in(jax.random.fold_in(stream_key, 6), dim), (shards_of,), jnp.float32, least / len(shards), top_value / len(shards))
        return jnp.repeat(jnp.exp(draws), dims[dim] // shards_of).reshape((-1,) + (1,) * (len(dims) - dim - 1))

    factor_of = one(*shards[0])
    for cut in shards[1:]:
        factor_of = factor_of * one(*cut)
    return factor_of


def shared_out(stream_key, own, number, rows, amount, top, limit, skew):
    sequence = jax.random.permutation(stream_key, amount)
    crowded, usual = portions_of(amount, rows * top, limit, skew, True), portions_of(amount, rows * top, limit, skew, False)
    places = jnp.arange(amount)

    def named(tallies, rotation):
        used = int((tallies > 0).sum())
        fixed = max(1, used // 4)
        shifted = fixed + (places - fixed + rotation * (used - fixed)) % max(1, amount - fixed)
        return jnp.zeros((amount,), jnp.int32).at[sequence[jnp.where(places < fixed, places, shifted)]].set(jnp.asarray(tallies, jnp.int32))

    tallies = jnp.where(number % 4 == 0, named(crowded, number // 4), named(usual, number - number // 4 - 1))
    mixed = jax.random.permutation(jax.random.fold_in(own, 3), amount)
    donor, sink = mixed[0:amount // 2 * 2:2], mixed[1:amount // 2 * 2:2]
    margin = jnp.minimum(tallies[donor] - 1, limit - tallies[sink]) // 2
    margin = jnp.where((donor == sequence[0]) | (sink == sequence[0]) | (tallies[sink] == 0), 0, jnp.maximum(margin, 0))
    shifted = jax.random.randint(jax.random.fold_in(own, 4), (amount // 2,), 0, 1 << 20) % (margin + 1)
    tallies = tallies.at[donor].add(-shifted).at[sink].add(shifted)
    items = jnp.searchsorted(jnp.cumsum(tallies), jnp.arange(rows * top), side="right").astype(jnp.int32)
    listing = items.reshape(top, rows).T
    listing = listing[jax.random.permutation(jax.random.fold_in(own, 1), rows)]
    rotation = jax.random.randint(jax.random.fold_in(own, 2), (rows, 1), 0, top)
    return jnp.take_along_axis(listing, (jnp.arange(top)[None, :] + rotation) % top, axis=1)


def portions_of(number_of, total, reach, skew, full):
    weights = [(1 << 20) // math.isqrt(rank ** skew) + 1 for rank in range(1, number_of + 1)]
    largest = reach if full else min(reach, max(-(-total // number_of), total * weights[0] // sum(weights)))
    least = 1 if total - largest >= number_of - 1 else 0
    counts, surplus = [largest] + [least] * (number_of - 1), total - largest - least * (number_of - 1)
    while surplus > 0:
        free = [i for i in range(1, number_of) if counts[i] < largest] or [i for i in range(1, number_of) if counts[i] < reach]
        mass, left = sum([weights[i] for i in free]), surplus
        for i in free:
            more = min(reach - counts[i], max(1, left * weights[i] // mass), surplus)
            counts[i] = counts[i] + more
            surplus = surplus - more
    return np.array(counts)


def normal_values(rng, dims, deviation, bound, shards=(), kind=jnp.bfloat16):
    drawn = deviation * jax.random.normal(rng, dims, jnp.float32)
    if shards:
        drawn = drawn * levels(rng, dims, shards, -0.22, 0.18)
    return jnp.clip(drawn, -bound, bound).astype(kind)


def setup_inputs(seed: int = 0, part: int = 0) -> dict:
    arg_keys = jax.random.split(jax.random.key(seed), 9)
    part_keys = jax.random.split(jax.random.fold_in(arg_keys[8], part), 9)
    tokens = normal_values(part_keys[0], (TOKENS, D), 1.0, 6.0, ((0, 4),))
    route_keys = jax.random.split(jax.random.fold_in(part_keys[1], 1), TOKENS // TOK_E)
    route_turns = jax.random.permutation(jax.random.fold_in(part_keys[1], 3), TOKENS // TOK_E)
    route = jax.vmap(lambda own, number: shared_out(jax.random.fold_in(part_keys[1], 2), own, number, TOK_E, EXPERTS, 1, CAP, 2))(route_keys, route_turns).reshape((TOKENS, 1))
    gate_prob = jnp.clip(jnp.exp(math.log(1.0) - 1.609438 * jax.random.uniform(part_keys[2], (TOKENS,), jnp.float32) ** levels(part_keys[2], (TOKENS,), ((0, 4),), -0.2, 0.2)), 0.2, 1.0)
    norm_gain = jnp.clip(1.0 + 0.1 * jax.random.normal(arg_keys[3], (D,), jnp.float32), 0.5, 1.5)
    dense_in = normal_values(arg_keys[4], (D, FF), D ** -0.5, 0.125, ((0, 4), (1, 4)))
    dense_out = normal_values(arg_keys[5], (FF, D), FF ** -0.5, 0.0625, ((0, 4), (1, 4)))
    expert_in = normal_values(arg_keys[6], (EXPERTS, D, FF), D ** -0.5, 0.125, ((0, 4), (2, 4)))
    expert_out = normal_values(arg_keys[7], (EXPERTS, FF, D), FF ** -0.5, 0.0625, ((0, 4), (1, 4)))
    return {"tokens": tokens, "route": route, "gate_prob": gate_prob, "norm_gain": norm_gain, "dense_in": dense_in, "dense_out": dense_out, "expert_in": expert_in, "expert_out": expert_out}


def normalize(tokens, norm_gain):
    widened = tokens.astype(jnp.float32)
    meansq = lax.optimization_barrier(jnp.mean(widened * widened, axis=-1, keepdims=True))
    return (widened * lax.rsqrt(meansq + 1e-06) * norm_gain).astype(jnp.bfloat16)

def sliced_product(act, weight):
    rows = act.shape[0]
    width = FF // N_CUTS
    act_parts = act.reshape(rows, N_CUTS, width).transpose(1, 0, 2)
    weight_parts = weight.reshape(N_CUTS, width, D)

    def add_slice(total, operands):
        act_part, weight_part = operands
        partial_out = jnp.dot(act_part, weight_part, preferred_element_type=jnp.float32)
        rounded = lax.optimization_barrier(partial_out.astype(jnp.bfloat16)).astype(jnp.float32)
        return (total + rounded, None)
    total, unused = lax.scan(add_slice, jnp.zeros((rows, D), jnp.float32), (act_parts, weight_parts))
    return total

def run_expert(operands):
    gathered, weight_in, weight_out = operands
    inner = jax.nn.gelu(jnp.dot(gathered, weight_in, preferred_element_type=jnp.float32)).astype(jnp.bfloat16)
    return sliced_product(inner, weight_out).astype(jnp.bfloat16)

def reference(tokens, route, gate_prob, norm_gain, dense_in, dense_out, expert_in, expert_out):
    normed = normalize(tokens, norm_gain)
    dense_act = jax.nn.gelu(jnp.dot(normed, dense_in, preferred_element_type=jnp.float32)).astype(jnp.bfloat16)
    dense = sliced_product(dense_act, dense_out)
    picked = route[:, 0].reshape(N_EXPERT, TOK_E)
    labels = jnp.arange(EXPERTS, dtype=jnp.int32)
    one_hot = (picked[:, :, None] == labels[None, None, :]).astype(jnp.int32)
    before = jnp.cumsum(one_hot, axis=1) - one_hot
    position = lax.optimization_barrier(jnp.sum(before * one_hot, axis=-1))
    block_ids = jnp.arange(N_EXPERT, dtype=jnp.int32)[:, None]
    target = (picked * (N_EXPERT * CAP) + block_ids * CAP + position).reshape(-1).astype(jnp.int32)
    buffer = jnp.zeros((EXPERTS * N_EXPERT * CAP, D), jnp.bfloat16).at[target].set(normed)
    buffer = buffer.reshape(EXPERTS, N_EXPERT * CAP, D)
    results = lax.map(run_expert, (buffer, expert_in, expert_out)).reshape(-1, D)
    expert_res = results[target].astype(jnp.float32)
    layer_out = tokens.astype(jnp.float32) + dense + gate_prob[:, None] * expert_res
    return layer_out.astype(jnp.bfloat16)
```

```python
import functools

import jax
import jax.numpy as jnp
from jax import lax
from jax.experimental import pallas as pl
from jax.experimental.pallas import tpu as pltpu
from jax.sharding import PartitionSpec as P

SUB = 4


def kernel(G, E, Z, cap, tokens, route, gate, gain, din, dout, ein_h, eout_h, out,
           win, wout, ein, eout, tok, normed, disp, arrived, hbuf, pe, rpe, pd, rpd, ret, rret,
           loc, own_s, own_r, disp_s, disp_r, wx_s, wx_r, wy_s, wy_r, wp_s, wp_r,
           ze_s, ze_r, zd_s, zd_r, ret_s, ret_r):
    f32, bf16 = jnp.float32, jnp.bfloat16
    T, D = tok.shape
    F = ein.shape[1]
    De = D // E
    share = D // Z
    C = E // 2
    pair = 2 * cap
    tn = min(256, share)
    g, e, z = lax.axis_index("groups"), lax.axis_index("expert"), lax.axis_index("cuts")
    chip, core = e // 2, lax.rem(e, 2)
    partner = chip * 2 + 1 - core

    def remote(src, dst, send, recv, gg=None, ee=None, zz=None):
        return pltpu.make_async_remote_copy(
            src_ref=src, dst_ref=dst, send_sem=send, recv_sem=recv,
            device_id={
                "groups": g if gg is None else gg,
                "expert": e if ee is None else ee,
                "cuts": z if zz is None else zz,
            },
            device_id_type=pl.DeviceIdType.MESH,
        )

    def expert_at(kc, j):
        other = lax.rem(chip + kc + C, C)
        return other * 2 + (core if j == 0 else 1 - core)

    barrier = pltpu.get_barrier_semaphore()
    for k in range(1, E):
        pl.semaphore_signal(barrier, inc=1, device_id={"groups": g, "expert": lax.rem(e + k, E), "cuts": z},
                            device_id_type=pl.DeviceIdType.MESH)
    for k in range(1, Z):
        pl.semaphore_signal(barrier, inc=1, device_id={"groups": g, "expert": e, "cuts": lax.rem(z + k, Z)},
                            device_id_type=pl.DeviceIdType.MESH)
    for k in range(1, G):
        pl.semaphore_signal(barrier, inc=1, device_id={"groups": lax.rem(g + k, G), "expert": e, "cuts": z},
                            device_id_type=pl.DeviceIdType.MESH)

    my_rows = pl.ds(pl.multiple_of(e * De, De), De)
    locals_ = [
        pltpu.make_async_copy(tokens, tok, loc.at[0]),
        pltpu.make_async_copy(ein_h.at[0], ein, loc.at[1]),
        pltpu.make_async_copy(eout_h.at[0], eout, loc.at[2]),
        pltpu.make_async_copy(din, win.at[my_rows, :], loc.at[3]),
        pltpu.make_async_copy(dout, wout.at[:, my_rows], loc.at[4]),
    ]
    for copy in locals_:
        copy.start()
    locals_[0].wait()

    nrow = min(64, T)

    def norm_step(i, carry):
        rows = pl.ds(pl.multiple_of(i * nrow, nrow), nrow)
        x = tok[rows, :].astype(f32)
        ms = jnp.mean(x * x, axis=-1, keepdims=True)
        normed[rows, :] = (x * lax.rsqrt(ms + 1e-06) * gain[...]).astype(bf16)
        return carry

    lax.fori_loop(0, T // nrow, norm_step, 0)

    picked = route[...]
    one_hot = (lax.broadcasted_iota(jnp.int32, (T, 128), 1) == picked).astype(f32)
    lower = (lax.broadcasted_iota(jnp.int32, (T, T), 1) < lax.broadcasted_iota(jnp.int32, (T, T), 0))
    before = jnp.dot(lower.astype(f32).astype(bf16), one_hot.astype(bf16), preferred_element_type=f32)
    position = jnp.sum(before * one_hot, axis=1, keepdims=True)
    slot_col = picked.astype(f32) * float(cap) + position
    slot_row = jnp.transpose(jnp.broadcast_to(slot_col, (T, 128)))[0:1, :]

    pl.semaphore_wait(barrier, (E - 1) + (Z - 1) + (G - 1))

    own_copies = [
        remote(din, win.at[my_rows, :], own_s.at[0], own_r.at[0], ee=partner),
        remote(dout, wout.at[:, my_rows], own_s.at[1], own_r.at[1], ee=partner),
    ]

    def fill(q, dst):
        dest = expert_at(q // 2, q % 2)
        wanted = slot_row - (dest * cap).astype(f32)
        pick = (lax.broadcasted_iota(jnp.int32, (cap, T), 0).astype(f32) == wanted).astype(f32).astype(bf16)
        dn = min(512, D)

        def step(i, carry):
            cols = pl.ds(pl.multiple_of(i * dn, dn), dn)
            dst[q * cap:(q + 1) * cap, cols] = jnp.dot(
                pick, normed[:, cols], preferred_element_type=f32).astype(bf16)
            return carry

        lax.fori_loop(0, D // dn, step, 0)

    def disp_copy(q):
        return remote(disp.at[pl.ds(q * cap, cap), :], arrived.at[pl.ds(q * cap, cap), :],
                      disp_s.at[q], disp_r.at[q], ee=expert_at(q // 2, q % 2))

    order = list(range(2, E)) + [1]
    pending = None
    for q in order:
        fill(q, disp)
        if pending is not None:
            disp_copy(pending).start()
        pending = q
    fill(0, arrived)
    disp_copy(pending).start()

    def in_at(owner, p, s):
        n = De // G // SUB
        return pl.ds(pl.multiple_of(owner * De + p * (De // G) + s * n, n), n)

    def weight(m, owner, p, s):
        if m == 0:
            n = De // G // SUB
            return win.at[pl.ds(pl.multiple_of(owner * De + p * (De // G) + s * n, n), n), :]
        n = F // G // SUB
        return wout.at[pl.ds(pl.multiple_of(p * (F // G) + s * n, n), n),
                       pl.ds(pl.multiple_of(owner * De, De), De)]

    def weight_source(m, p, s):
        ref, rows = (din, De) if m == 0 else (dout, F)
        n = rows // G // SUB
        return ref.at[pl.ds(pl.multiple_of(p * (rows // G) + s * n, n), n), :]

    def x_copy(m, kc, s):
        return remote(weight_source(m, g, s), weight(m, e, g, s), wx_s.at[m, kc, s], wx_r.at[m, kc, s],
                      ee=expert_at(kc, 0))

    def y_copy(m, kc, s, dg):
        w = weight(m, expert_at(-kc, 0), g, s)
        return remote(w, w, wy_s.at[m, kc, s, dg], wy_r.at[m, kc, s, dg], gg=lax.rem(g + dg, G))

    def p_copy(m, kc, s, dg):
        w = weight(m, expert_at(-kc, 0), lax.rem(g - dg + G, G), s)
        return remote(w, w, wp_s.at[m, kc, s, dg], wp_r.at[m, kc, s, dg], ee=partner)

    for m in range(2):
        for s in range(SUB):
            for kc in range(1, C):
                x_copy(m, kc, s).start()
    for copy in own_copies:
        copy.start()

    def ze_copy(kc, r):
        rows = pl.ds(kc * pair, pair)
        return remote(pe.at[r, rows, :], rpe.at[r, rows, :], ze_s.at[kc, r], ze_r.at[kc, r],
                      zz=lax.rem(z + r, Z))

    def zd_copy(r):
        return remote(pd.at[r], rpd.at[r], zd_s.at[r], zd_r.at[r], zz=lax.rem(z + r, Z))

    def hidden(load, rows, w):
        def step(i, carry):
            cols = pl.ds(pl.multiple_of(i * 256, 256), 256)
            acc = jnp.dot(load(), w[:, cols], preferred_element_type=f32)
            hbuf[0:rows, cols] = jax.nn.gelu(acc).astype(bf16)
            return carry

        lax.fori_loop(0, F // 256, step, 0)

    def partials(rows, w, store, send):
        late = None
        for r in list(range(Z - 1, 0, -1)) + [0]:
            base = lax.rem(z + r, Z) * share

            def step(i, carry):
                cols = pl.ds(pl.multiple_of(base + i * tn, tn), tn)
                acc = jnp.dot(hbuf[0:rows, :], w[:, cols], preferred_element_type=f32)
                store(r, pl.ds(pl.multiple_of(i * tn, tn), tn), acc.astype(bf16))
                return carry

            lax.fori_loop(0, share // tn, step, 0)
            if late is not None:
                send(late).start()
            late = r

    locals_[1].wait()
    locals_[2].wait()
    for kc in range(C):
        for q in (2 * kc, 2 * kc + 1):
            if q:
                disp_copy(q).wait_recv()
        lo = kc * pair
        hidden(lambda: arrived[lo:lo + pair, :], pair, ein)

        def store(r, cols, value):
            pe[r, lo:lo + pair, cols] = value

        partials(pair, eout, store, lambda r: ze_copy(kc, r))

    def forward(m):
        for s in range(SUB):
            for kc in range(1, C):
                x_copy(m, kc, s).wait_recv()
                for dg in range(1, G):
                    y_copy(m, kc, s, dg).start()
                p_copy(m, kc, s, 0).start()
            if s:
                forward_group(m, s - 1)
        forward_group(m, SUB - 1)

    def forward_group(m, s):
        for kc in range(1, C):
            for dg in range(1, G):
                y_copy(m, kc, s, dg).wait_recv()
                p_copy(m, kc, s, dg).start()

    def collect(m):
        locals_[3 + m].wait()
        own_copies[m].wait_recv()
        for s in range(SUB):
            for kc in range(1, C):
                for dg in range(G):
                    p_copy(m, kc, s, dg).wait_recv()

    forward(0)
    collect(0)
    hidden(lambda: normed[...], T, win)
    forward(1)
    collect(1)

    def store_dense(r, cols, value):
        pd[r, :, cols] = value

    partials(T, wout, store_dense, zd_copy)

    def ret_copy(q):
        return remote(ret.at[pl.ds(q * cap, cap), :], rret.at[pl.ds(q * cap, cap), :],
                      ret_s.at[q], ret_r.at[q], ee=expert_at(-(q // 2), q % 2))

    for kc in list(range(1, C)) + [0]:
        lo = kc * pair
        for r in range(1, Z):
            ze_copy(kc, r).wait_recv()
        for q in (2 * kc + 1, 2 * kc):
            rows = slice(q * cap, (q + 1) * cap)
            total = pe[0, rows, :].astype(f32)
            for r in range(1, Z):
                total = total + rpe[r, rows, :].astype(f32)
            if q:
                ret[rows, :] = total.astype(bf16)
            else:
                rret[rows, :] = total.astype(bf16)
        for q in (2 * kc, 2 * kc + 1):
            if q:
                ret_copy(q).start()

    for q in range(1, E):
        ret_copy(q).wait_recv()

    for r in range(1, Z):
        zd_copy(r).wait_recv()

    trow = min(128, T)
    residual = pl.ds(pl.multiple_of(z * share, share), share)
    for i in range(T // trow):
        rows = slice(i * trow, (i + 1) * trow)
        res = jnp.zeros((trow, share), f32)
        for q in range(E):
            wanted = slot_col[rows, :] - (expert_at(q // 2, q % 2) * cap).astype(f32)
            pick = (lax.broadcasted_iota(jnp.int32, (trow, cap), 1).astype(f32) == wanted).astype(f32).astype(bf16)
            res = res + jnp.dot(pick, rret[q * cap:(q + 1) * cap, :], preferred_element_type=f32)
        dense = pd[0, rows, :].astype(f32)
        for r in range(1, Z):
            dense = dense + rpd[r, rows, :].astype(f32)
        out[rows, :] = (tok[rows, residual].astype(f32) + dense + gate[rows, :] * res).astype(bf16)

    for copy in own_copies:
        copy.wait_send()
    for q in range(1, E):
        disp_copy(q).wait_send()
        ret_copy(q).wait_send()
    for m in range(2):
        for s in range(SUB):
            for kc in range(1, C):
                x_copy(m, kc, s).wait_send()
                for dg in range(1, G):
                    y_copy(m, kc, s, dg).wait_send()
                for dg in range(G):
                    p_copy(m, kc, s, dg).wait_send()
    for r in range(1, Z):
        for kc in range(C):
            ze_copy(kc, r).wait_send()
        zd_copy(r).wait_send()


def local(tokens, route, gate_prob, norm_gain, dense_in, dense_out, expert_in, expert_out):
    G, E, Z = lax.axis_size("groups"), lax.axis_size("expert"), lax.axis_size("cuts")
    T, D = tokens.shape
    F = dense_in.shape[1]
    share = D // Z
    cap = max(2, 3 * T // (2 * E))
    C = E // 2
    bf16 = jnp.bfloat16
    any_, vmem = pl.BlockSpec(memory_space=pl.ANY), pl.BlockSpec(memory_space=pltpu.VMEM)
    dma = pltpu.SemaphoreType.DMA
    return pl.pallas_call(
        functools.partial(kernel, G, E, Z, cap),
        out_shape=jax.ShapeDtypeStruct((T, share), bf16),
        in_specs=[any_, vmem, vmem, vmem, any_, any_, any_, any_],
        out_specs=vmem,
        scratch_shapes=[
            pltpu.VMEM((D, F), bf16), pltpu.VMEM((F, D), bf16),
            pltpu.VMEM((D, F), bf16), pltpu.VMEM((F, D), bf16),
            pltpu.VMEM((T, D), bf16), pltpu.VMEM((T, D), bf16),
            pltpu.VMEM((E * cap, D), bf16), pltpu.VMEM((E * cap, D), bf16),
            pltpu.VMEM((max(T, 2 * cap), F), bf16),
            pltpu.VMEM((Z, E * cap, share), bf16), pltpu.VMEM((Z, E * cap, share), bf16),
            pltpu.VMEM((Z, T, share), bf16), pltpu.VMEM((Z, T, share), bf16),
            pltpu.VMEM((E * cap, share), bf16), pltpu.VMEM((E * cap, share), bf16),
            dma((5,)), dma((2,)), dma((2,)), dma((E,)), dma((E,)),
            dma((2, C, SUB)), dma((2, C, SUB)),
            dma((2, C, SUB, G)), dma((2, C, SUB, G)), dma((2, C, SUB, G)), dma((2, C, SUB, G)),
            dma((C, Z)), dma((C, Z)), dma((Z,)), dma((Z,)), dma((E,)), dma((E,)),
        ],
        compiler_params=pltpu.CompilerParams(
            collective_id=0, has_side_effects=True, vmem_limit_bytes=67043328
        ),
    )(tokens, route, gate_prob[:, None], norm_gain[None, :], dense_in, dense_out, expert_in, expert_out)


def solution(mesh):
    return jax.shard_map(
        local,
        mesh=mesh,
        in_specs=(
            P(("groups", "expert"), None),
            P(("groups", "expert"), None),
            P(("groups", "expert")),
            P(),
            P("expert", "cuts"),
            P("cuts", "expert"),
            P("expert", None, "cuts"),
            P("expert", "cuts", None),
        ),
        out_specs=P(("groups", "expert"), "cuts"),
        check_vma=False,
    )
```

```python
import functools

import jax
import jax.numpy as jnp
from jax import lax
from jax.experimental import pallas as pl
from jax.experimental.pallas import tpu as pltpu
from jax.sharding import PartitionSpec as P

SUBS = (4, 4)
WINDOW = 3
EARLY = 1


def kernel(G, E, Z, cap, tokens, route, gate, gain, din, dout, ein_h, eout_h, out,
           win, wout, ein, eout, tok, normed, disp, arrived, hbuf, pe, rpe, pd, rpd, ret, rret,
           loc, own_s, own_r, disp_s, disp_r, wx_s, wx_r, wy_s, wy_r, wp_s, wp_r,
           ze_s, ze_r, zd_s, zd_r, ret_s, ret_r):
    f32, bf16 = jnp.float32, jnp.bfloat16
    T, D = tok.shape
    F = ein.shape[1]
    De = D // E
    share = D // Z
    C = E // 2
    pair = 2 * cap
    tn = min(256, share)
    g, e, z = lax.axis_index("groups"), lax.axis_index("expert"), lax.axis_index("cuts")
    chip, core = e // 2, lax.rem(e, 2)
    partner = chip * 2 + 1 - core

    def remote(src, dst, send, recv, gg=None, ee=None, zz=None):
        return pltpu.make_async_remote_copy(
            src_ref=src, dst_ref=dst, send_sem=send, recv_sem=recv,
            device_id={
                "groups": g if gg is None else gg,
                "expert": e if ee is None else ee,
                "cuts": z if zz is None else zz,
            },
            device_id_type=pl.DeviceIdType.MESH,
        )

    def expert_at(kc, j):
        other = lax.rem(chip + kc + C, C)
        return other * 2 + (core if j == 0 else 1 - core)

    barrier = pltpu.get_barrier_semaphore()
    for k in range(1, E):
        pl.semaphore_signal(barrier, inc=1, device_id={"groups": g, "expert": lax.rem(e + k, E), "cuts": z},
                            device_id_type=pl.DeviceIdType.MESH)
    for k in range(1, Z):
        pl.semaphore_signal(barrier, inc=1, device_id={"groups": g, "expert": e, "cuts": lax.rem(z + k, Z)},
                            device_id_type=pl.DeviceIdType.MESH)
    for k in range(1, G):
        pl.semaphore_signal(barrier, inc=1, device_id={"groups": lax.rem(g + k, G), "expert": e, "cuts": z},
                            device_id_type=pl.DeviceIdType.MESH)

    my_rows = pl.ds(pl.multiple_of(e * De, De), De)
    locals_ = [
        pltpu.make_async_copy(tokens, tok, loc.at[0]),
        pltpu.make_async_copy(ein_h.at[0], ein, loc.at[1]),
        pltpu.make_async_copy(eout_h.at[0], eout, loc.at[2]),
        pltpu.make_async_copy(din, win.at[my_rows, :], loc.at[3]),
        pltpu.make_async_copy(dout, wout.at[:, my_rows], loc.at[4]),
    ]
    for copy in locals_:
        copy.start()
    pl.semaphore_wait(barrier, (E - 1) + (Z - 1) + (G - 1))

    own_copies = [
        remote(din, win.at[my_rows, :], own_s.at[0], own_r.at[0], ee=partner),
        remote(dout, wout.at[:, my_rows], own_s.at[1], own_r.at[1], ee=partner),
    ]

    def weight(m, owner, p, s):
        if m == 0:
            n = De // G // SUBS[m]
            return win.at[pl.ds(pl.multiple_of(owner * De + p * (De // G) + s * n, n), n), :]
        n = F // G // SUBS[m]
        return wout.at[pl.ds(pl.multiple_of(p * (F // G) + s * n, n), n),
                       pl.ds(pl.multiple_of(owner * De, De), De)]

    def weight_source(m, p, s):
        ref, rows = (din, De) if m == 0 else (dout, F)
        n = rows // G // SUBS[m]
        return ref.at[pl.ds(pl.multiple_of(p * (rows // G) + s * n, n), n), :]

    def x_copy(m, kc, s):
        return remote(weight_source(m, g, s), weight(m, e, g, s), wx_s.at[m, kc, s], wx_r.at[m, kc, s],
                      ee=expert_at(kc, 0))

    def y_copy(m, kc, s, dg):
        w = weight(m, expert_at(-kc, 0), g, s)
        return remote(w, w, wy_s.at[m, kc, s, dg], wy_r.at[m, kc, s, dg], gg=lax.rem(g + dg, G))

    def p_copy(m, kc, s, dg):
        w = weight(m, expert_at(-kc, 0), lax.rem(g - dg + G, G), s)
        return remote(w, w, wp_s.at[m, kc, s, dg], wp_r.at[m, kc, s, dg], ee=partner)

    steps = [(m, s) for m in range(2) for s in range(SUBS[m])]
    issued, taken, relayed = [0], [0], [0]

    def issue(upto):
        while issued[0] < min(upto, len(steps)):
            m, s = steps[issued[0]]
            for kc in range(1, C):
                x_copy(m, kc, s).start()
            issued[0] += 1

    def relay():
        m, s = steps[relayed[0]]
        for kc in range(1, C):
            for dg in range(1, G):
                y_copy(m, kc, s, dg).wait_recv()
                p_copy(m, kc, s, dg).start()
        relayed[0] += 1

    def take(upto):
        while taken[0] < min(upto, len(steps)):
            m, s = steps[taken[0]]
            for kc in range(1, C):
                x_copy(m, kc, s).wait_recv()
            if taken[0] >= EARLY:
                issue(taken[0] + 1 + WINDOW)
            for kc in range(1, C):
                for dg in range(1, G):
                    y_copy(m, kc, s, dg).start()
                p_copy(m, kc, s, 0).start()
            if relayed[0] < taken[0]:
                relay()
            taken[0] += 1

    issue(EARLY)
    locals_[0].wait()

    nrow = min(64, T)

    def norm_step(i, carry):
        rows = pl.ds(pl.multiple_of(i * nrow, nrow), nrow)
        x = tok[rows, :].astype(f32)
        ms = jnp.mean(x * x, axis=-1, keepdims=True)
        normed[rows, :] = (x * lax.rsqrt(ms + 1e-06) * gain[...]).astype(bf16)
        return carry

    lax.fori_loop(0, T // nrow, norm_step, 0)

    picked = route[...]
    one_hot = (lax.broadcasted_iota(jnp.int32, (T, 128), 1) == picked).astype(f32)
    lower = (lax.broadcasted_iota(jnp.int32, (T, T), 1) < lax.broadcasted_iota(jnp.int32, (T, T), 0))
    before = jnp.dot(lower.astype(f32).astype(bf16), one_hot.astype(bf16), preferred_element_type=f32)
    position = jnp.sum(before * one_hot, axis=1, keepdims=True)
    slot_col = picked.astype(f32) * float(cap) + position
    slot_row = jnp.transpose(jnp.broadcast_to(slot_col, (T, 128)))[0:1, :]

    def fill(q, dst):
        dest = expert_at(q // 2, q % 2)
        wanted = slot_row - (dest * cap).astype(f32)
        pick = (lax.broadcasted_iota(jnp.int32, (cap, T), 0).astype(f32) == wanted).astype(f32).astype(bf16)
        dn = min(512, D)

        def step(i, carry):
            cols = pl.ds(pl.multiple_of(i * dn, dn), dn)
            dst[q * cap:(q + 1) * cap, cols] = jnp.dot(
                pick, normed[:, cols], preferred_element_type=f32).astype(bf16)
            return carry

        lax.fori_loop(0, D // dn, step, 0)

    def disp_copy(q):
        return remote(disp.at[pl.ds(q * cap, cap), :], arrived.at[pl.ds(q * cap, cap), :],
                      disp_s.at[q], disp_r.at[q], ee=expert_at(q // 2, q % 2))

    order = list(range(2, E)) + [1]
    pending = None
    for q in order:
        fill(q, disp)
        if pending is not None:
            disp_copy(pending).start()
        pending = q
    fill(0, arrived)
    disp_copy(pending).start()

    for copy in own_copies:
        copy.start()

    def ze_copy(kc, r):
        rows = pl.ds(kc * pair, pair)
        return remote(pe.at[r, rows, :], rpe.at[r, rows, :], ze_s.at[kc, r], ze_r.at[kc, r],
                      zz=lax.rem(z + r, Z))

    halfrows = T // 2

    def zd_copy(d, slot, c, to):
        rows = pl.ds(c * halfrows, halfrows)
        return remote(pd.at[d, rows, :], rpd.at[slot, rows, :], zd_s.at[d, c], zd_r.at[slot, c], zz=to)

    def back_slot(d, to):
        return Z if d == to else d

    def hidden(load, rows, w, lo=0, hi=None):
        def step(i, carry):
            cols = pl.ds(pl.multiple_of(i * 256, 256), 256)
            acc = jnp.dot(load(), w[:, cols], preferred_element_type=f32)
            hbuf[0:rows, cols] = jax.nn.gelu(acc).astype(bf16)
            return carry

        lax.fori_loop(lo, F // 256 if hi is None else hi, step, 0)

    def partials(rows, w, store, send):
        late = None
        for r in list(range(Z - 1, 0, -1)) + [0]:
            base = lax.rem(z + r, Z) * share

            def step(i, carry):
                cols = pl.ds(pl.multiple_of(base + i * tn, tn), tn)
                acc = jnp.dot(hbuf[0:rows, :], w[:, cols], preferred_element_type=f32)
                store(r, pl.ds(pl.multiple_of(i * tn, tn), tn), acc.astype(bf16))
                return carry

            lax.fori_loop(0, share // tn, step, 0)
            if late is not None:
                send(late).start()
            late = r

    locals_[1].wait()
    locals_[2].wait()
    for kc in range(C):
        for q in (2 * kc, 2 * kc + 1):
            if q:
                disp_copy(q).wait_recv()
        if kc == C - 1:
            issue(EARLY + WINDOW)
        lo = kc * pair
        hidden(lambda: arrived[lo:lo + pair, :], pair, ein)

        def store(r, cols, value):
            pe[r, lo:lo + pair, cols] = value

        partials(pair, eout, store, lambda r: ze_copy(kc, r))
        if kc == 0:
            take(EARLY)

    def collect(m):
        locals_[3 + m].wait()
        own_copies[m].wait_recv()
        for s in range(SUBS[m]):
            for kc in range(1, C):
                for dg in range(G):
                    p_copy(m, kc, s, dg).wait_recv()

    first = SUBS[0]
    take(first + 1)
    while relayed[0] < first:
        relay()
    collect(0)
    blocks = F // 256
    for part in range(4):
        hidden(lambda: normed[...], T, win, part * blocks // 4, (part + 1) * blocks // 4)
        take(first + 2 + part)
    take(len(steps))
    while relayed[0] < len(steps):
        relay()
    collect(1)

    upper = (2 * z) // Z
    for i in range(Z):
        d = (1 - upper) * (Z - 1 - i) + upper * i

        def dense_step(k, carry):
            cols = pl.ds(pl.multiple_of(d * share + k * tn, tn), tn)
            acc = jnp.dot(hbuf[0:T, :], wout[:, cols], preferred_element_type=f32)
            pd[d, :, pl.ds(pl.multiple_of(k * tn, tn), tn)] = acc.astype(bf16)
            return carry

        lax.fori_loop(0, share // tn, dense_step, 0)
        if i < Z - 1:
            @pl.when(z == 0)
            def _():
                for c in range(2):
                    zd_copy(Z - 1 - i, Z - 1 - i, c, 1).start()

            @pl.when(z == Z - 1)
            def _():
                for c in range(2):
                    zd_copy(i, back_slot(i, Z - 2), c, Z - 2).start()

    def ret_copy(q):
        return remote(ret.at[pl.ds(q * cap, cap), :], rret.at[pl.ds(q * cap, cap), :],
                      ret_s.at[q], ret_r.at[q], ee=expert_at(-(q // 2), q % 2))

    for kc in list(range(1, C)) + [0]:
        lo = kc * pair
        for r in range(1, Z):
            ze_copy(kc, r).wait_recv()
        for q in (2 * kc + 1, 2 * kc):
            rows = slice(q * cap, (q + 1) * cap)
            total = pe[0, rows, :].astype(f32)
            for r in range(1, Z):
                total = total + rpe[r, rows, :].astype(f32)
            if q:
                ret[rows, :] = total.astype(bf16)
            else:
                rret[rows, :] = total.astype(bf16)
        for q in (2 * kc, 2 * kc + 1):
            if q:
                ret_copy(q).start()

    def add_arrived(d, c):
        rows = slice(c * halfrows, (c + 1) * halfrows)
        pd[d, rows, :] = (pd[d, rows, :].astype(f32) + rpd[d, rows, :].astype(f32)).astype(bf16)

    for t in range(Z - 1):
        for c in range(2):
            up, down = Z - 1 - t, t

            @pl.when((z > 0) & (z < up))
            def _():
                zd_copy(up, up, c, lax.rem(z + 1, Z)).wait_recv()
                add_arrived(up, c)
                zd_copy(up, up, c, lax.rem(z + 1, Z)).start()

            @pl.when((z < Z - 1) & (z > down + 1))
            def _():
                zd_copy(down, down, c, lax.rem(z + Z - 1, Z)).wait_recv()
                add_arrived(down, c)
                zd_copy(down, down, c, lax.rem(z + Z - 1, Z)).start()

            @pl.when((z < Z - 1) & (z == down + 1))
            def _():
                zd_copy(down, down, c, lax.rem(z + Z - 1, Z)).wait_recv()
                add_arrived(down, c)
                zd_copy(down, Z, c, lax.rem(z + Z - 1, Z)).start()

    for q in range(1, E):
        ret_copy(q).wait_recv()

    @pl.when(z == 0)
    def _():
        rpd[0] = jnp.zeros((T, share), bf16)

    @pl.when(z == Z - 1)
    def _():
        rpd[Z] = jnp.zeros((T, share), bf16)

    for c in range(2):
        @pl.when(z > 0)
        def _():
            zd_copy(z, z, c, lax.rem(z + 1, Z)).wait_recv()

        @pl.when(z < Z - 1)
        def _():
            zd_copy(z, Z, c, lax.rem(z + 1, Z)).wait_recv()

    trow = min(128, T)
    residual = pl.ds(pl.multiple_of(z * share, share), share)
    for i in range(T // trow):
        rows = slice(i * trow, (i + 1) * trow)
        res = jnp.zeros((trow, share), f32)
        for q in range(E):
            wanted = slot_col[rows, :] - (expert_at(q // 2, q % 2) * cap).astype(f32)
            pick = (lax.broadcasted_iota(jnp.int32, (trow, cap), 1).astype(f32) == wanted).astype(f32).astype(bf16)
            res = res + jnp.dot(pick, rret[q * cap:(q + 1) * cap, :], preferred_element_type=f32)
        dense = pd[z, rows, :].astype(f32) + rpd[z, rows, :].astype(f32) + rpd[Z, rows, :].astype(f32)
        out[rows, :] = (tok[rows, residual].astype(f32) + dense + gate[rows, :] * res).astype(bf16)

    for copy in own_copies:
        copy.wait_send()
    for q in range(1, E):
        disp_copy(q).wait_send()
        ret_copy(q).wait_send()
    for m in range(2):
        for s in range(SUBS[m]):
            for kc in range(1, C):
                x_copy(m, kc, s).wait_send()
                for dg in range(1, G):
                    y_copy(m, kc, s, dg).wait_send()
                for dg in range(G):
                    p_copy(m, kc, s, dg).wait_send()
    for r in range(1, Z):
        for kc in range(C):
            ze_copy(kc, r).wait_send()
    for d in range(Z):
        @pl.when(z != d)
        def _():
            for c in range(2):
                zd_copy(d, d, c, lax.rem(z + 1, Z)).wait_send()


def local(tokens, route, gate_prob, norm_gain, dense_in, dense_out, expert_in, expert_out):
    G, E, Z = lax.axis_size("groups"), lax.axis_size("expert"), lax.axis_size("cuts")
    T, D = tokens.shape
    F = dense_in.shape[1]
    share = D // Z
    cap = max(2, 3 * T // (2 * E))
    C = E // 2
    bf16 = jnp.bfloat16
    any_, vmem = pl.BlockSpec(memory_space=pl.ANY), pl.BlockSpec(memory_space=pltpu.VMEM)
    dma = pltpu.SemaphoreType.DMA
    return pl.pallas_call(
        functools.partial(kernel, G, E, Z, cap),
        out_shape=jax.ShapeDtypeStruct((T, share), bf16),
        in_specs=[any_, vmem, vmem, vmem, any_, any_, any_, any_],
        out_specs=vmem,
        scratch_shapes=[
            pltpu.VMEM((D, F), bf16), pltpu.VMEM((F, D), bf16),
            pltpu.VMEM((D, F), bf16), pltpu.VMEM((F, D), bf16),
            pltpu.VMEM((T, D), bf16), pltpu.VMEM((T, D), bf16),
            pltpu.VMEM((E * cap, D), bf16), pltpu.VMEM((E * cap, D), bf16),
            pltpu.VMEM((max(T, 2 * cap), F), bf16),
            pltpu.VMEM((Z, E * cap, share), bf16), pltpu.VMEM((Z, E * cap, share), bf16),
            pltpu.VMEM((Z, T, share), bf16), pltpu.VMEM((Z + 1, T, share), bf16),
            pltpu.VMEM((E * cap, share), bf16), pltpu.VMEM((E * cap, share), bf16),
            dma((5,)), dma((2,)), dma((2,)), dma((E,)), dma((E,)),
            dma((2, C, max(SUBS))), dma((2, C, max(SUBS))),
            dma((2, C, max(SUBS), G)), dma((2, C, max(SUBS), G)), dma((2, C, max(SUBS), G)), dma((2, C, max(SUBS), G)),
            dma((C, Z)), dma((C, Z)), dma((Z, 2)), dma((Z + 1, 2)), dma((E,)), dma((E,)),
        ],
        compiler_params=pltpu.CompilerParams(
            collective_id=0, has_side_effects=True, vmem_limit_bytes=67043328
        ),
    )(tokens, route, gate_prob[:, None], norm_gain[None, :], dense_in, dense_out, expert_in, expert_out)


def solution(mesh):
    return jax.shard_map(
        local,
        mesh=mesh,
        in_specs=(
            P(("groups", "expert"), None),
            P(("groups", "expert"), None),
            P(("groups", "expert")),
            P(),
            P("expert", "cuts"),
            P("cuts", "expert"),
            P("expert", None, "cuts"),
            P("expert", "cuts", None),
        ),
        out_specs=P(("groups", "expert"), "cuts"),
        check_vma=False,
    )
```

```python
import functools

import jax
import jax.numpy as jnp
from jax import lax
from jax.experimental import pallas as pl
from jax.experimental.pallas import tpu as pltpu
from jax.sharding import PartitionSpec as P

SUBS = (4, 4)
WINDOW = 3
EARLY = 1


def kernel(G, E, Z, cap, tokens, route, gate, gain, din, dout, ein_h, eout_h, out,
           win, wout, ein, eout, tok, normed, disp, arrived, hbuf, pe, rpe, pd, rpd, ret, rret, base,
           loc, own_s, own_r, disp_s, disp_r, wx_s, wx_r, wy_s, wy_r, wp_s, wp_r,
           ze_s, ze_r, zd_s, zd_r, ret_s, ret_r):
    f32, bf16 = jnp.float32, jnp.bfloat16
    T, D = tok.shape
    F = ein.shape[1]
    De = D // E
    share = D // Z
    C = E // 2
    pair = 2 * cap
    tn = min(256, share)
    g, e, z = lax.axis_index("groups"), lax.axis_index("expert"), lax.axis_index("cuts")
    chip, core = e // 2, lax.rem(e, 2)
    partner = chip * 2 + 1 - core

    def remote(src, dst, send, recv, gg=None, ee=None, zz=None):
        return pltpu.make_async_remote_copy(
            src_ref=src, dst_ref=dst, send_sem=send, recv_sem=recv,
            device_id={
                "groups": g if gg is None else gg,
                "expert": e if ee is None else ee,
                "cuts": z if zz is None else zz,
            },
            device_id_type=pl.DeviceIdType.MESH,
        )

    def expert_at(kc, j):
        other = lax.rem(chip + kc + C, C)
        return other * 2 + (core if j == 0 else 1 - core)

    barrier = pltpu.get_barrier_semaphore()
    for k in range(1, E):
        pl.semaphore_signal(barrier, inc=1, device_id={"groups": g, "expert": lax.rem(e + k, E), "cuts": z},
                            device_id_type=pl.DeviceIdType.MESH)
    for k in range(1, Z):
        pl.semaphore_signal(barrier, inc=1, device_id={"groups": g, "expert": e, "cuts": lax.rem(z + k, Z)},
                            device_id_type=pl.DeviceIdType.MESH)
    for k in range(1, G):
        pl.semaphore_signal(barrier, inc=1, device_id={"groups": lax.rem(g + k, G), "expert": e, "cuts": z},
                            device_id_type=pl.DeviceIdType.MESH)

    my_rows = pl.ds(pl.multiple_of(e * De, De), De)
    locals_ = [
        pltpu.make_async_copy(tokens, tok, loc.at[0]),
        pltpu.make_async_copy(ein_h.at[0], ein, loc.at[1]),
        pltpu.make_async_copy(eout_h.at[0], eout, loc.at[2]),
        pltpu.make_async_copy(din, win.at[my_rows, :], loc.at[3]),
        pltpu.make_async_copy(dout, wout.at[:, my_rows], loc.at[4]),
    ]
    for copy in locals_:
        copy.start()
    pl.semaphore_wait(barrier, (E - 1) + (Z - 1) + (G - 1))

    own_copies = [
        remote(din, win.at[my_rows, :], own_s.at[0], own_r.at[0], ee=partner),
        remote(dout, wout.at[:, my_rows], own_s.at[1], own_r.at[1], ee=partner),
    ]

    def weight(m, owner, p, s):
        if m == 0:
            n = De // G // SUBS[m]
            return win.at[pl.ds(pl.multiple_of(owner * De + p * (De // G) + s * n, n), n), :]
        n = F // G // SUBS[m]
        return wout.at[pl.ds(pl.multiple_of(p * (F // G) + s * n, n), n),
                       pl.ds(pl.multiple_of(owner * De, De), De)]

    def weight_source(m, p, s):
        ref, rows = (din, De) if m == 0 else (dout, F)
        n = rows // G // SUBS[m]
        return ref.at[pl.ds(pl.multiple_of(p * (rows // G) + s * n, n), n), :]

    def x_copy(m, kc, s):
        return remote(weight_source(m, g, s), weight(m, e, g, s), wx_s.at[m, kc, s], wx_r.at[m, kc, s],
                      ee=expert_at(kc, 0))

    def y_copy(m, kc, s, dg):
        w = weight(m, expert_at(-kc, 0), g, s)
        return remote(w, w, wy_s.at[m, kc, s, dg], wy_r.at[m, kc, s, dg], gg=lax.rem(g + dg, G))

    def p_copy(m, kc, s, dg):
        w = weight(m, expert_at(-kc, 0), lax.rem(g - dg + G, G), s)
        return remote(w, w, wp_s.at[m, kc, s, dg], wp_r.at[m, kc, s, dg], ee=partner)

    steps = [(m, s) for m in range(2) for s in range(SUBS[m])]
    issued, taken, relayed = [0], [0], [0]

    def issue(upto):
        while issued[0] < min(upto, len(steps)):
            m, s = steps[issued[0]]
            for kc in range(1, C):
                x_copy(m, kc, s).start()
            issued[0] += 1

    def relay():
        m, s = steps[relayed[0]]
        for kc in range(1, C):
            for dg in range(1, G):
                y_copy(m, kc, s, dg).wait_recv()
                p_copy(m, kc, s, dg).start()
        relayed[0] += 1

    def take(upto):
        while taken[0] < min(upto, len(steps)):
            m, s = steps[taken[0]]
            for kc in range(1, C):
                x_copy(m, kc, s).wait_recv()
            if taken[0] >= EARLY:
                issue(taken[0] + 1 + WINDOW)
            for kc in range(1, C):
                for dg in range(1, G):
                    y_copy(m, kc, s, dg).start()
                p_copy(m, kc, s, 0).start()
            if relayed[0] < taken[0]:
                relay()
            taken[0] += 1

    issue(EARLY)
    locals_[0].wait()

    nrow = min(64, T)

    def norm_step(i, carry):
        rows = pl.ds(pl.multiple_of(i * nrow, nrow), nrow)
        x = tok[rows, :].astype(f32)
        ms = jnp.mean(x * x, axis=-1, keepdims=True)
        normed[rows, :] = (x * lax.rsqrt(ms + 1e-06) * gain[...]).astype(bf16)
        return carry

    lax.fori_loop(0, T // nrow, norm_step, 0)

    picked = route[...]
    one_hot = (lax.broadcasted_iota(jnp.int32, (T, 128), 1) == picked).astype(f32)
    lower = (lax.broadcasted_iota(jnp.int32, (T, T), 1) < lax.broadcasted_iota(jnp.int32, (T, T), 0))
    before = jnp.dot(lower.astype(f32).astype(bf16), one_hot.astype(bf16), preferred_element_type=f32)
    position = jnp.sum(before * one_hot, axis=1, keepdims=True)
    slot_col = picked.astype(f32) * float(cap) + position
    slot_row = jnp.transpose(jnp.broadcast_to(slot_col, (T, 128)))[0:1, :]

    def fill(q, dst):
        dest = expert_at(q // 2, q % 2)
        wanted = slot_row - (dest * cap).astype(f32)
        pick = (lax.broadcasted_iota(jnp.int32, (cap, T), 0).astype(f32) == wanted).astype(f32).astype(bf16)
        dn = min(512, D)

        def step(i, carry):
            cols = pl.ds(pl.multiple_of(i * dn, dn), dn)
            dst[q * cap:(q + 1) * cap, cols] = jnp.dot(
                pick, normed[:, cols], preferred_element_type=f32).astype(bf16)
            return carry

        lax.fori_loop(0, D // dn, step, 0)

    def disp_copy(q):
        return remote(disp.at[pl.ds(q * cap, cap), :], arrived.at[pl.ds(q * cap, cap), :],
                      disp_s.at[q], disp_r.at[q], ee=expert_at(q // 2, q % 2))

    order = list(range(2, E)) + [1]
    pending = None
    for q in order:
        fill(q, disp)
        if pending is not None:
            disp_copy(pending).start()
        pending = q
    fill(0, arrived)
    disp_copy(pending).start()

    for copy in own_copies:
        copy.start()

    def ze_copy(kc, r):
        rows = pl.ds(kc * pair, pair)
        return remote(pe.at[r, rows, :], rpe.at[r, rows, :], ze_s.at[kc, r], ze_r.at[kc, r],
                      zz=lax.rem(z + r, Z))

    halfrows = T // 2

    def zd_copy(d, slot, c, to):
        rows = pl.ds(c * halfrows, halfrows)
        return remote(pd.at[d, rows, :], rpd.at[slot, rows, :], zd_s.at[d, c], zd_r.at[slot, c], zz=to)

    def back_slot(d, to):
        return Z if d == to else d

    def hidden(load, rows, w, lo=0, hi=None):
        def step(i, carry):
            cols = pl.ds(pl.multiple_of(i * 256, 256), 256)
            acc = jnp.dot(load(), w[:, cols], preferred_element_type=f32)
            hbuf[0:rows, cols] = jax.nn.gelu(acc).astype(bf16)
            return carry

        lax.fori_loop(lo, F // 256 if hi is None else hi, step, 0)

    def partials(rows, w, store, send):
        late = None
        for r in list(range(Z - 1, 0, -1)) + [0]:
            base = lax.rem(z + r, Z) * share

            def step(i, carry):
                cols = pl.ds(pl.multiple_of(base + i * tn, tn), tn)
                acc = jnp.dot(hbuf[0:rows, :], w[:, cols], preferred_element_type=f32)
                store(r, pl.ds(pl.multiple_of(i * tn, tn), tn), acc.astype(bf16))
                return carry

            lax.fori_loop(0, share // tn, step, 0)
            if late is not None:
                send(late).start()
            late = r

    locals_[1].wait()
    locals_[2].wait()
    for kc in range(C):
        for q in (2 * kc, 2 * kc + 1):
            if q:
                disp_copy(q).wait_recv()
        if kc == C - 1:
            issue(EARLY + WINDOW)
        lo = kc * pair
        hidden(lambda: arrived[lo:lo + pair, :], pair, ein)

        def store(r, cols, value):
            pe[r, lo:lo + pair, cols] = value

        partials(pair, eout, store, lambda r: ze_copy(kc, r))
        if kc == 0:
            take(EARLY)

    def collect(m):
        locals_[3 + m].wait()
        own_copies[m].wait_recv()
        for s in range(SUBS[m]):
            for kc in range(1, C):
                for dg in range(G):
                    p_copy(m, kc, s, dg).wait_recv()

    first = SUBS[0]
    take(first + 1)
    while relayed[0] < first:
        relay()
    collect(0)
    blocks = F // 256
    for part in range(4):
        hidden(lambda: normed[...], T, win, part * blocks // 4, (part + 1) * blocks // 4)
        take(first + 2 + part)
    take(len(steps))
    while relayed[0] < len(steps):
        relay()
    collect(1)

    upper = (2 * z) // Z
    for i in range(Z):
        d = (1 - upper) * (Z - 1 - i) + upper * i

        def dense_step(k, carry):
            cols = pl.ds(pl.multiple_of(d * share + k * tn, tn), tn)
            acc = jnp.dot(hbuf[0:T, :], wout[:, cols], preferred_element_type=f32)
            pd[d, :, pl.ds(pl.multiple_of(k * tn, tn), tn)] = acc.astype(bf16)
            return carry

        lax.fori_loop(0, share // tn, dense_step, 0)
        if i < Z - 1:
            @pl.when(z == 0)
            def _():
                for c in range(2):
                    zd_copy(Z - 1 - i, Z - 1 - i, c, 1).start()

            @pl.when(z == Z - 1)
            def _():
                for c in range(2):
                    zd_copy(i, back_slot(i, Z - 2), c, Z - 2).start()

    def ret_copy(q):
        return remote(ret.at[pl.ds(q * cap, cap), :], rret.at[pl.ds(q * cap, cap), :],
                      ret_s.at[q], ret_r.at[q], ee=expert_at(-(q // 2), q % 2))

    for kc in list(range(1, C)) + [0]:
        lo = kc * pair
        for r in range(1, Z):
            ze_copy(kc, r).wait_recv()
        for q in (2 * kc + 1, 2 * kc):
            rows = slice(q * cap, (q + 1) * cap)
            total = pe[0, rows, :].astype(f32)
            for r in range(1, Z):
                total = total + rpe[r, rows, :].astype(f32)
            if q:
                ret[rows, :] = total.astype(bf16)
            else:
                rret[rows, :] = total.astype(bf16)
        for q in (2 * kc, 2 * kc + 1):
            if q:
                ret_copy(q).start()

    def add_arrived(d, c):
        rows = slice(c * halfrows, (c + 1) * halfrows)
        pd[d, rows, :] = (pd[d, rows, :].astype(f32) + rpd[d, rows, :].astype(f32)).astype(bf16)

    trow = min(128, T)
    residual = pl.ds(pl.multiple_of(z * share, share), share)

    def combine_experts():
        for q in range(1, E):
            ret_copy(q).wait_recv()
        for i in range(T // trow):
            rows = slice(i * trow, (i + 1) * trow)
            res = jnp.zeros((trow, share), f32)
            for q in range(E):
                wanted = slot_col[rows, :] - (expert_at(q // 2, q % 2) * cap).astype(f32)
                pick = (lax.broadcasted_iota(jnp.int32, (trow, cap), 1).astype(f32) == wanted)
                res = res + jnp.dot(pick.astype(f32).astype(bf16), rret[q * cap:(q + 1) * cap, :],
                                    preferred_element_type=f32)
            base[rows, :] = tok[rows, residual].astype(f32) + gate[rows, :] * res

    above, below = lax.rem(z + 1, Z), lax.rem(z + Z - 1, Z)

    def pass_up(d, c):
        @pl.when((z > 0) & (z < d))
        def _():
            zd_copy(d, d, c, above).wait_recv()
            add_arrived(d, c)
            zd_copy(d, d, c, above).start()

    def pass_down(d, c):
        for slot, near in ((d, z > d + 1), (Z, z == d + 1)):
            @pl.when((z < Z - 1) & near)
            def _():
                zd_copy(d, d, c, below).wait_recv()
                add_arrived(d, c)
                zd_copy(d, slot, c, below).start()

    for t in range(Z - 1):
        @pl.when(upper == 0)
        def _():
            for c in range(2):
                pass_up(Z - 1 - t, c)
            for c in range(2):
                pass_down(t, c)

        @pl.when(upper == 1)
        def _():
            for c in range(2):
                pass_down(t, c)
            for c in range(2):
                pass_up(Z - 1 - t, c)

        if t == 0:
            combine_experts()

    @pl.when(z == 0)
    def _():
        rpd[0] = jnp.zeros((T, share), bf16)

    @pl.when(z == Z - 1)
    def _():
        rpd[Z] = jnp.zeros((T, share), bf16)

    for c in range(2):
        @pl.when(z > 0)
        def _():
            zd_copy(z, z, c, lax.rem(z + 1, Z)).wait_recv()

        @pl.when(z < Z - 1)
        def _():
            zd_copy(z, Z, c, lax.rem(z + 1, Z)).wait_recv()

    for i in range(T // trow):
        rows = slice(i * trow, (i + 1) * trow)
        dense = pd[z, rows, :].astype(f32) + rpd[z, rows, :].astype(f32) + rpd[Z, rows, :].astype(f32)
        out[rows, :] = (base[rows, :] + dense).astype(bf16)

    for copy in own_copies:
        copy.wait_send()
    for q in range(1, E):
        disp_copy(q).wait_send()
        ret_copy(q).wait_send()
    for m in range(2):
        for s in range(SUBS[m]):
            for kc in range(1, C):
                x_copy(m, kc, s).wait_send()
                for dg in range(1, G):
                    y_copy(m, kc, s, dg).wait_send()
                for dg in range(G):
                    p_copy(m, kc, s, dg).wait_send()
    for r in range(1, Z):
        for kc in range(C):
            ze_copy(kc, r).wait_send()
    for d in range(Z):
        @pl.when(z != d)
        def _():
            for c in range(2):
                zd_copy(d, d, c, lax.rem(z + 1, Z)).wait_send()


def local(tokens, route, gate_prob, norm_gain, dense_in, dense_out, expert_in, expert_out):
    G, E, Z = lax.axis_size("groups"), lax.axis_size("expert"), lax.axis_size("cuts")
    T, D = tokens.shape
    F = dense_in.shape[1]
    share = D // Z
    cap = max(2, 3 * T // (2 * E))
    C = E // 2
    bf16 = jnp.bfloat16
    any_, vmem = pl.BlockSpec(memory_space=pl.ANY), pl.BlockSpec(memory_space=pltpu.VMEM)
    dma = pltpu.SemaphoreType.DMA
    return pl.pallas_call(
        functools.partial(kernel, G, E, Z, cap),
        out_shape=jax.ShapeDtypeStruct((T, share), bf16),
        in_specs=[any_, vmem, vmem, vmem, any_, any_, any_, any_],
        out_specs=vmem,
        scratch_shapes=[
            pltpu.VMEM((D, F), bf16), pltpu.VMEM((F, D), bf16),
            pltpu.VMEM((D, F), bf16), pltpu.VMEM((F, D), bf16),
            pltpu.VMEM((T, D), bf16), pltpu.VMEM((T, D), bf16),
            pltpu.VMEM((E * cap, D), bf16), pltpu.VMEM((E * cap, D), bf16),
            pltpu.VMEM((max(T, 2 * cap), F), bf16),
            pltpu.VMEM((Z, E * cap, share), bf16), pltpu.VMEM((Z, E * cap, share), bf16),
            pltpu.VMEM((Z, T, share), bf16), pltpu.VMEM((Z + 1, T, share), bf16),
            pltpu.VMEM((E * cap, share), bf16), pltpu.VMEM((E * cap, share), bf16),
            pltpu.VMEM((T, share), jnp.float32),
            dma((5,)), dma((2,)), dma((2,)), dma((E,)), dma((E,)),
            dma((2, C, max(SUBS))), dma((2, C, max(SUBS))),
            dma((2, C, max(SUBS), G)), dma((2, C, max(SUBS), G)), dma((2, C, max(SUBS), G)), dma((2, C, max(SUBS), G)),
            dma((C, Z)), dma((C, Z)), dma((Z, 2)), dma((Z + 1, 2)), dma((E,)), dma((E,)),
        ],
        compiler_params=pltpu.CompilerParams(
            collective_id=0, has_side_effects=True, vmem_limit_bytes=67043328
        ),
    )(tokens, route, gate_prob[:, None], norm_gain[None, :], dense_in, dense_out, expert_in, expert_out)


def solution(mesh):
    return jax.shard_map(
        local,
        mesh=mesh,
        in_specs=(
            P(("groups", "expert"), None),
            P(("groups", "expert"), None),
            P(("groups", "expert")),
            P(),
            P("expert", "cuts"),
            P("cuts", "expert"),
            P("expert", None, "cuts"),
            P("expert", "cuts", None),
        ),
        out_specs=P(("groups", "expert"), "cuts"),
        check_vma=False,
    )
```
